32 devices in a mesh: dp: 1 (over z), b: 4 (over y), cp: 8 (over x, core).
Axes of the slice: x: 4, y: 4, z: 1, core: 2. Of those that a mesh axis runs over, the one named last changes fastest.
The devices are a block of a 4x4x8 slice.
Arguments:
- x: bfloat16 [48, 768, 2048], P(('dp', 'b'), 'cp')
- ids: int32 [48, 768, 6], P(('dp', 'b'), 'cp')
- g_attn: bfloat16 [2048], replicated
- w_q: bfloat16 [2048, 3072], replicated
- w_dkv: bfloat16 [2048, 512], replicated
- w_kr: bfloat16 [2048, 64], replicated
- w_uk: bfloat16 [16, 128, 512], replicated
- w_uv: bfloat16 [16, 512, 128], replicated
- w_o: bfloat16 [2048, 2048], replicated
- g_ffn: bfloat16 [2048], replicated
- w_fg: bfloat16 [2048, 10944], replicated
- w_fu: bfloat16 [2048, 10944], replicated
- w_fd: bfloat16 [10944, 2048], replicated
- g_moe: bfloat16 [2048], replicated
- w_r: bfloat16 [2048, 96], replicated
- w_eg: bfloat16 [64, 2048, 1408], P(('b', 'cp'))
- w_eu: bfloat16 [64, 2048, 1408], P(('b', 'cp'))
- w_ed: bfloat16 [64, 1408, 2048], P(('b', 'cp'))
Outputs:
- output: bfloat16 [48, 768, 2048], P(('dp', 'b'), 'cp')
All inputs are finite; a program needn't handle non-finite values.
Results may differ from the reference program's by a relative error of at most 0.00874767.
Values are sent between devices in bfloat16 or wider.
A program may use at most 768 MiB of HBM per device.

```python
import jax
import jax.numpy as jnp
from jax import lax

D = 2048
HEADS = 16
R = 512
EXPERTS = 64
TOP = 6
EFF = 1408
FF = 10944
ROWS = 12
SEQ = 96
NB = 4
NC = 8
NOPE = 128
ROPE = 64
VDIM = 128

B = ROWS * NB
S = SEQ * NC
T = B * S
TBLK = ROWS * SEQ
NSLOT = EXPERTS + EXPERTS // 2
WIDTH = NSLOT // TOP
HOT = WIDTH // 2
CAP = (TBLK + HOT - 1) // HOT
CAPALL = NB * NC * CAP
EPS = 1e-6
SCALE = (NOPE + ROPE) ** -0.5


def _nrm(k, shape, scale):
    return (jax.random.normal(k, shape, jnp.float32) * scale).astype(jnp.bfloat16)


def _gain(k):
    return jax.random.uniform(k, (D,), jnp.float32, 0.6, 1.4).astype(jnp.bfloat16)


def setup_inputs(seed: int = 0, part: int = 0) -> dict:
    kp = jax.random.fold_in(jax.random.key(seed), part)
    kw = jax.random.split(jax.random.key(seed + 1), 16)
    k1, k2, k3, k4, k5 = jax.random.split(kp, 5)
    pos = jnp.arange(S, dtype=jnp.float32) / S
    amp = jax.random.normal(k2, (B, 3, D), jnp.float32) * 0.6
    phase = jax.random.uniform(k3, (B, 3, 1), jnp.float32, 0.0, 6.2832)
    freq = jnp.arange(1, 4, dtype=jnp.float32).reshape(1, 3, 1)
    wave = jnp.cos(6.2832 * freq * pos.reshape(1, 1, S) + phase)
    x = 0.7 * jax.random.normal(k1, (B, S, D), jnp.float32) + jnp.einsum('clt,cle->cte', wave, amp)
    ka, kb, kc = jax.random.split(jax.random.fold_in(kp, 7), 3)
    shift = jax.random.randint(ka, (), 0, NSLOT)
    perm = (jnp.arange(NSLOT) + shift) % NSLOT
    tperm = jax.vmap(lambda kk: jax.random.permutation(kk, TBLK))(jax.random.split(kb, NB * NC * TOP))
    off = jax.random.randint(kc, (NB * NC * TOP, 1), 0, WIDTH - HOT + 1)
    r = (tperm % HOT + off).reshape(NB, NC, TOP, TBLK)
    slot = jnp.arange(TOP).reshape(1, 1, TOP, 1) * WIDTH + r
    ids = perm[slot].reshape(NB, NC, TOP, ROWS, SEQ).transpose(0, 3, 1, 4, 2).reshape(B, S, TOP)
    return {
        'x': x.astype(jnp.bfloat16),
        'ids': ids.astype(jnp.int32),
        'g_attn': _gain(kw[0]),
        'w_q': _nrm(kw[1], (D, HEADS * (NOPE + ROPE)), D ** -0.5),
        'w_dkv': _nrm(kw[2], (D, R), D ** -0.5),
        'w_kr': _nrm(kw[3], (D, ROPE), D ** -0.5),
        'w_uk': _nrm(kw[4], (HEADS, NOPE, R), 0.5 * NOPE ** -0.5),
        'w_uv': _nrm(kw[5], (HEADS, R, VDIM), R ** -0.5),
        'w_o': _nrm(kw[6], (HEADS * VDIM, D), (HEADS * VDIM) ** -0.5),
        'g_ffn': _gain(kw[7]),
        'w_fg': _nrm(kw[8], (D, FF), D ** -0.5),
        'w_fu': _nrm(kw[9], (D, FF), D ** -0.5),
        'w_fd': _nrm(kw[10], (FF, D), FF ** -0.5),
        'g_moe': _gain(kw[11]),
        'w_r': _nrm(kw[12], (D, NSLOT), 2.0 * D ** -0.5),
        'w_eg': _nrm(kw[13], (EXPERTS, D, EFF), D ** -0.5),
        'w_eu': _nrm(kw[14], (EXPERTS, D, EFF), D ** -0.5),
        'w_ed': _nrm(kw[15], (EXPERTS, EFF, D), 2.0 * EFF ** -0.5),
    }


def _rms(v, g):
    vf = v.astype(jnp.float32)
    return (vf * lax.rsqrt(jnp.mean(vf * vf, axis=-1, keepdims=True) + EPS) * g.astype(jnp.float32)).astype(jnp.bfloat16)


def _rope(v, cos, sin):
    half = ROPE // 2
    v1 = v[..., :half]
    v2 = v[..., half:]
    return jnp.concatenate([v1 * cos - v2 * sin, v1 * sin + v2 * cos], axis=-1)


def _swiglu(z, wg, wu, wd):
    hid = jax.nn.silu(jnp.dot(z, wg, preferred_element_type=jnp.float32)) * jnp.dot(z, wu, preferred_element_type=jnp.float32)
    return jnp.dot(hid.astype(jnp.bfloat16), wd, preferred_element_type=jnp.float32).astype(jnp.bfloat16)


def reference(x, ids, g_attn, w_q, w_dkv, w_kr, w_uk, w_uv, w_o, g_ffn, w_fg, w_fu, w_fd, g_moe, w_r, w_eg, w_eu, w_ed):
    pos = jnp.arange(S)
    half = ROPE // 2
    ang = pos.astype(jnp.float32)[:, None] * (10000.0 ** (-jnp.arange(half, dtype=jnp.float32) / half))[None, :]
    cos = jnp.cos(ang)
    sin = jnp.sin(ang)
    causal = pos[:, None] >= pos[None, :]

    def attn_row(xr):
        n = _rms(xr, g_attn)
        c = jnp.dot(n, w_dkv, preferred_element_type=jnp.float32).astype(jnp.bfloat16)
        kr = _rope(jnp.dot(n, w_kr, preferred_element_type=jnp.float32), cos, sin).astype(jnp.bfloat16)
        q = jnp.dot(n, w_q, preferred_element_type=jnp.float32).reshape(S, HEADS, NOPE + ROPE)
        qn = q[..., :NOPE].astype(jnp.bfloat16)
        qt = jnp.einsum('shn,hnr->shr', qn.astype(jnp.float32), w_uk.astype(jnp.float32)).astype(jnp.bfloat16)
        qr = _rope(q[..., NOPE:], cos[:, None, :], sin[:, None, :]).astype(jnp.bfloat16)

        def head(hargs):
            qh, qrh, wuv = hargs
            sc = (jnp.dot(qh, c.T, preferred_element_type=jnp.float32) + jnp.dot(qrh, kr.T, preferred_element_type=jnp.float32)) * SCALE
            sc = jnp.where(causal, sc, -jnp.inf)
            p = jnp.exp(sc - jnp.max(sc, axis=-1, keepdims=True))
            lat = (jnp.dot(p.astype(jnp.bfloat16), c, preferred_element_type=jnp.float32) / jnp.sum(p, axis=-1, keepdims=True)).astype(jnp.bfloat16)
            return jnp.dot(lat, wuv, preferred_element_type=jnp.float32).astype(jnp.bfloat16)

        o = lax.map(head, (jnp.transpose(qt, (1, 0, 2)), jnp.transpose(qr, (1, 0, 2)), w_uv))
        o = jnp.transpose(o, (1, 0, 2)).reshape(S, HEADS * VDIM)
        return jnp.dot(o, w_o, preferred_element_type=jnp.float32).astype(jnp.bfloat16)

    a = lax.map(attn_row, x)
    y = (x.astype(jnp.float32) + a.astype(jnp.float32)).astype(jnp.bfloat16)
    n2 = _rms(y, g_ffn).reshape(B * NC, SEQ, D)
    f = lax.map(lambda z: _swiglu(z, w_fg, w_fu, w_fd), n2).reshape(T, D)
    u = _rms(x, g_moe).reshape(T, D)
    idf = ids.reshape(T, TOP)
    g = jax.nn.softmax(jnp.dot(u, w_r, preferred_element_type=jnp.float32), axis=-1)
    sel = jnp.take_along_axis(g, idf, axis=1)
    gate = sel / jnp.sum(sel, axis=1, keepdims=True)
    gflat = gate.reshape(-1)
    flat = idf.reshape(-1)
    order = jnp.argsort(flat, stable=True)
    starts = jnp.searchsorted(flat[order], jnp.arange(EXPERTS + 1, dtype=flat.dtype))
    zero = jnp.sum(jnp.where(idf >= EXPERTS, gate, 0.0), axis=1)
    m0 = zero[:, None] * u.astype(jnp.float32)

    def expert(m, eargs):
        e, wg, wu, wd = eargs
        k = starts[e] + jnp.arange(CAPALL)
        slot = order[jnp.minimum(k, T * TOP - 1)]
        tok = slot // TOP
        out = _swiglu(u[tok], wg, wu, wd)
        w = jnp.where(k < starts[e + 1], gflat[slot], 0.0)
        return m.at[tok].add(w[:, None] * out.astype(jnp.float32)), None

    m, _ = lax.scan(expert, m0, (jnp.arange(EXPERTS), w_eg, w_eu, w_ed))
    h = y.reshape(T, D).astype(jnp.float32) + f.astype(jnp.float32) + m
    return h.astype(jnp.bfloat16).reshape(B, S, D)
```

```python
import functools

import jax
import jax.numpy as jnp
from jax import lax
from jax.experimental import pallas as pl
from jax.experimental.pallas import tpu as pltpu
from jax.sharding import PartitionSpec as P

NOPE = 128
ROPE = 64
EPS = 1e-6
SCALE = (NOPE + ROPE) ** -0.5
F32 = jnp.float32
BF16 = jnp.bfloat16
LANE = 128
VMEM_MAX = 67043328


def _rms(v, g):
    vf = v.astype(F32)
    return (vf * lax.rsqrt(jnp.mean(vf * vf, axis=-1, keepdims=True) + EPS) * g.astype(F32)).astype(BF16)


def _rope(v, cos, sin):
    half = ROPE // 2
    v1 = v[..., :half]
    v2 = v[..., half:]
    return jnp.concatenate([v1 * cos - v2 * sin, v1 * sin + v2 * cos], axis=-1)


def _swiglu(z, wg, wu, wd):
    hid = jax.nn.silu(jnp.dot(z, wg, preferred_element_type=F32)) * jnp.dot(z, wu, preferred_element_type=F32)
    return jnp.dot(hid.astype(BF16), wd, preferred_element_type=F32).astype(BF16)


def _gates(u, ids, w_r):
    g = jax.nn.softmax(jnp.dot(u, w_r, preferred_element_type=F32), axis=-1)
    hit = ids[:, :, None] == jnp.arange(g.shape[1], dtype=ids.dtype)
    sel = jnp.sum(jnp.where(hit, g[:, None, :], 0.0), axis=2)
    return sel / jnp.sum(sel, axis=1, keepdims=True)


def _rope_tables(pos):
    half = ROPE // 2
    ang = pos.astype(F32)[:, None] * (10000.0 ** (-jnp.arange(half, dtype=F32) / half))[None, :]
    return jnp.cos(ang), jnp.sin(ang)


def _attn_kernel(off_ref, qt_ref, qr_ref, kv_ref, o_ref):
    hg, seq, r = qt_ref.shape
    blocks = kv_ref.shape[0]
    keys = blocks * seq
    kv = kv_ref[...].reshape(keys, kv_ref.shape[-1])
    c = kv[:, :r]
    kr = kv[:, r:]
    nt = (((1,), (1,)), ((), ()))
    s = lax.dot_general(qt_ref[...].reshape(hg * seq, r), c, nt, preferred_element_type=F32)
    s = s + lax.dot_general(qr_ref[...].reshape(hg * seq, qr_ref.shape[-1]), kr, nt, preferred_element_type=F32)
    s = (s * SCALE).reshape(hg, seq, keys)
    query = off_ref[0] + lax.broadcasted_iota(jnp.int32, (1, seq, keys), 1)
    key = lax.broadcasted_iota(jnp.int32, (1, seq, keys), 2)
    s = jnp.where(key <= query, s, -jnp.inf).reshape(hg * seq, keys)
    p = jnp.exp(s - jnp.max(s, axis=-1, keepdims=True))
    den = jnp.sum(p, axis=-1, keepdims=True)
    lat = jnp.dot(p.astype(BF16), c, preferred_element_type=F32) / den
    o_ref[...] = lat.astype(BF16).reshape(hg, seq, r)


def _attention(off, qt, qr, kv, hg):
    heads, rows, seq, r = qt.shape
    e = qr.shape[-1]
    blocks = kv.shape[0]
    return pl.pallas_call(
        _attn_kernel,
        grid_spec=pltpu.PrefetchScalarGridSpec(
            num_scalar_prefetch=1,
            grid=(rows, heads // hg),
            in_specs=[
                pl.BlockSpec((hg, None, seq, r), lambda b, g, _: (g, b, 0, 0)),
                pl.BlockSpec((hg, None, seq, e), lambda b, g, _: (g, b, 0, 0)),
                pl.BlockSpec((blocks, None, seq, r + e), lambda b, g, _: (0, b, 0, 0)),
            ],
            out_specs=pl.BlockSpec((hg, None, seq, r), lambda b, g, _: (g, b, 0, 0)),
        ),
        out_shape=jax.ShapeDtypeStruct(qt.shape, BF16),
        compiler_params=pltpu.CompilerParams(vmem_limit_bytes=VMEM_MAX, dimension_semantics=("arbitrary", "arbitrary")),
        cost_estimate=pl.CostEstimate(
            flops=2 * heads * rows * seq * blocks * seq * (2 * r + e),
            bytes_accessed=2 * (2 * qt.size + qr.size + kv.size),
            transcendentals=heads * rows * seq * blocks * seq),
        name="latent_attention",
    )(off, qt, qr, kv)


def _scatter_kernel(top, pos_ref, u_ref, *rest):
    outs, buf, sem = rest[:-2], rest[-2], rest[-1]
    t, d = u_ref.shape
    k = d // LANE
    cap = outs[0].shape[0]
    step = 16

    def tok(i, _):
        base = pl.multiple_of(i * step, step)
        blk = u_ref[pl.ds(base, step), :].reshape(step, k, LANE)
        for a in range(step):
            row = blk[a]
            for j in range(top):
                buf[pos_ref[(base + a) * top + j]] = row
        return 0

    lax.fori_loop(0, t // step, tok, 0)
    copies = [pltpu.make_async_copy(buf.at[pl.ds(s * cap, cap)], outs[s], sem.at[s]) for s in range(len(outs))]
    for c in copies:
        c.start()
    for c in copies:
        c.wait()


def _scatter(u, pos, epd, cap, top):
    t, d = u.shape
    k = d // LANE
    return pl.pallas_call(
        functools.partial(_scatter_kernel, top),
        grid_spec=pltpu.PrefetchScalarGridSpec(
            num_scalar_prefetch=1,
            grid=(1,),
            in_specs=[pl.BlockSpec((t, d), lambda i, *_: (0, 0), pipeline_mode=pl.Buffered(1))],
            out_specs=[pl.BlockSpec(memory_space=pl.ANY)] * epd,
            scratch_shapes=[pltpu.VMEM((epd * cap + 8, k, LANE), BF16), pltpu.SemaphoreType.DMA((epd,))],
        ),
        out_shape=[jax.ShapeDtypeStruct((cap, k, LANE), BF16)] * epd,
        compiler_params=pltpu.CompilerParams(vmem_limit_bytes=VMEM_MAX),
        cost_estimate=pl.CostEstimate(flops=2 * 10**9, bytes_accessed=2 * (epd * cap + t) * d, transcendentals=0),
        name="scatter_rows",
    )(pos, u)


def _expert_kernel(x_ref, wg_ref, wu_ref, wd_ref, o_ref):
    tile = x_ref.shape[0]
    x = x_ref[...].reshape(tile, wg_ref.shape[0])
    g = jnp.dot(x, wg_ref[...], preferred_element_type=F32)
    v = jnp.dot(x, wu_ref[...], preferred_element_type=F32)
    hid = (jax.nn.silu(g) * v).astype(BF16)
    o = jnp.dot(hid, wd_ref[...], preferred_element_type=F32).astype(BF16)
    o_ref[...] = o.reshape(o_ref.shape)


def _expert(xs, w_eg, w_eu, w_ed, e, tile):
    cap, k, _ = xs.shape
    d, f = w_eg.shape[1:]
    one = pl.Buffered(1)
    row = pl.BlockSpec((tile, k, LANE), lambda i: (i, 0, 0))
    return pl.pallas_call(
        _expert_kernel,
        grid=(cap // tile,),
        in_specs=[
            row,
            pl.BlockSpec((None, d, f), lambda i: (e, 0, 0), pipeline_mode=one),
            pl.BlockSpec((None, d, f), lambda i: (e, 0, 0), pipeline_mode=one),
            pl.BlockSpec((None, f, d), lambda i: (e, 0, 0), pipeline_mode=one),
        ],
        out_specs=row,
        out_shape=jax.ShapeDtypeStruct(xs.shape, BF16),
        compiler_params=pltpu.CompilerParams(vmem_limit_bytes=VMEM_MAX, dimension_semantics=("arbitrary",)),
        cost_estimate=pl.CostEstimate(flops=6 * cap * d * f, bytes_accessed=6 * d * f + 4 * cap * d, transcendentals=cap * f),
        name=f"expert{e}",
    )(xs, w_eg, w_eu, w_ed)


def _combine_kernel(top, pos_ref, gate_ref, z_ref, y_ref, f_ref, u_ref, *rest):
    epd = len(rest) - 3
    rets, o_ref, buf, sem = rest[:epd], rest[epd], rest[epd + 1], rest[epd + 2]
    cap = rets[0].shape[0]
    tb, d = y_ref.shape
    k = d // LANE
    step = 16

    @pl.when(pl.program_id(0) == 0)
    def _():
        copies = [pltpu.make_async_copy(rets[s], buf.at[pl.ds(s * cap, cap)], sem.at[s]) for s in range(epd)]
        for c in copies:
            c.start()
        buf[pl.ds(epd * cap, 8)] = jnp.zeros((8, k, LANE), BF16)
        for c in copies:
            c.wait()

    first = pl.program_id(0) * tb

    def tok(i, _):
        base = pl.multiple_of(i * step, step)
        accs = []
        for a in range(step):
            acc = None
            for j in range(top):
                q = (first + base + a) * top + j
                term = buf[pos_ref[q]].astype(F32) * gate_ref[q]
                acc = term if acc is None else acc + term
            accs.append(acc)
        m = jnp.stack(accs).reshape(step, d)
        sl = pl.ds(base, step)
        m = m + z_ref[sl, :] * u_ref[sl, :].astype(F32)
        o_ref[sl, :] = (y_ref[sl, :].astype(F32) + f_ref[sl, :].astype(F32) + m).astype(BF16)
        return 0

    lax.fori_loop(0, tb // step, tok, 0)


def _combine(rets, y, f, u, pos, gate, zero, top):
    t, d = y.shape
    cap, k, _ = rets[0].shape
    epd = len(rets)
    tb = 128
    row = pl.BlockSpec((tb, d), lambda i, *_: (i, 0))
    return pl.pallas_call(
        functools.partial(_combine_kernel, top),
        grid_spec=pltpu.PrefetchScalarGridSpec(
            num_scalar_prefetch=2,
            grid=(t // tb,),
            in_specs=[pl.BlockSpec((tb, 1), lambda i, *_: (i, 0)), row, row, row] + [pl.BlockSpec(memory_space=pl.ANY)] * epd,
            out_specs=row,
            scratch_shapes=[pltpu.VMEM((epd * cap + 8, k, LANE), BF16), pltpu.SemaphoreType.DMA((epd,))],
        ),
        out_shape=jax.ShapeDtypeStruct((t, d), BF16),
        compiler_params=pltpu.CompilerParams(vmem_limit_bytes=VMEM_MAX, dimension_semantics=("arbitrary",)),
        cost_estimate=pl.CostEstimate(flops=2 * 10**9, bytes_accessed=2 * (epd * cap + 4 * t) * d, transcendentals=0),
        name="combine_rows",
    )(pos, gate, zero, y, f, u, *rets)


def solution(mesh):
    ncp = mesh.shape['cp']
    ngroup = mesh.shape['b'] * ncp
    axes = ('b', 'cp')
    tok = P(('dp', 'b'), 'cp', None)
    rep = P()
    espec = P(('b', 'cp'), None, None)

    def body(x, ids, g_attn, w_q, w_dkv, w_kr, w_uk, w_uv, w_o, g_ffn, w_fg, w_fu, w_fd, g_moe, w_r, w_eg, w_eu, w_ed):
        rows, seq, d = x.shape
        heads, r, vd = w_uv.shape
        top = ids.shape[-1]
        t = rows * seq
        epd = w_eg.shape[0]
        ne = epd * ngroup
        hot = (w_r.shape[1] // top) // 2
        per = (t + hot - 1) // hot
        cap = ngroup * per
        i = lax.axis_index('cp')
        xt = x.reshape(t, d)
        idf = ids.reshape(t, top)

        off = i * seq
        cos, sin = _rope_tables(off + jnp.arange(seq))
        n = _rms(xt, g_attn)
        c = jnp.dot(n, w_dkv, preferred_element_type=F32).astype(BF16).reshape(rows, seq, r)
        kr = _rope(jnp.dot(n, w_kr, preferred_element_type=F32).reshape(rows, seq, ROPE), cos, sin).astype(BF16)
        kv = lax.all_gather(jnp.concatenate([c, kr], axis=-1), 'cp')

        oh = idf[:, :, None] == jnp.arange(ne, dtype=idf.dtype)
        hit = jnp.any(oh, axis=1)
        k = jnp.arange(t)
        tri = (k[:, None] > k[None, :]).astype(BF16)
        pre = jnp.dot(tri, hit.astype(BF16), preferred_element_type=F32).astype(jnp.int32)
        e = jnp.arange(ne, dtype=jnp.int32)
        at = pre + ((e % epd) * cap + (e // epd) * per)[None, :]
        pos = jnp.sum(jnp.where(oh, at[:, None, :], 0), axis=2)
        pos = jnp.where(idf < ne, pos, epd * cap).reshape(t * top)

        u = _rms(xt, g_moe)
        send = _scatter(u, pos, epd, cap, top)
        got = []
        for s in range(epd):
            blk = send[s].reshape(ngroup, per, d // LANE, LANE)
            if s:
                blk, _ = lax.optimization_barrier((blk, got[-1]))
            got.append(lax.all_to_all(blk, axes, 0, 0))

        w_qh = w_q.reshape(d, heads, NOPE + ROPE)
        qn = jnp.dot(n, w_qh[..., :NOPE].reshape(d, heads * NOPE), preferred_element_type=F32).astype(BF16)
        qr = jnp.dot(n, w_qh[..., NOPE:].reshape(d, heads * ROPE), preferred_element_type=F32)
        qr = jnp.transpose(qr.reshape(rows, seq, heads, ROPE), (2, 0, 1, 3))
        qr = _rope(qr, cos, sin).astype(BF16)
        qt = jnp.einsum('thn,hnr->htr', qn.reshape(t, heads, NOPE), w_uk, preferred_element_type=F32).astype(BF16)
        lat = _attention(jnp.reshape(off, (1,)).astype(jnp.int32), qt.reshape(heads, rows, seq, r), qr, kv, heads // 2)
        o = jnp.einsum('htr,hrv->thv', lat.reshape(heads, t, r), w_uv, preferred_element_type=F32).astype(BF16)
        a = jnp.dot(o.reshape(t, heads * vd), w_o, preferred_element_type=F32).astype(BF16)
        y = (xt.astype(F32) + a.astype(F32)).astype(BF16)
        f = _swiglu(_rms(y, g_ffn), w_fg, w_fu, w_fd)

        gate = _gates(u, idf, w_r)
        ret = []
        for s in range(epd):
            out = _expert(got[s].reshape(cap, d // LANE, LANE), w_eg, w_eu, w_ed, s, 512)
            ret.append(lax.all_to_all(out.reshape(ngroup, per, d // LANE, LANE), axes, 0, 0).reshape(cap, d // LANE, LANE))
        ffn = idf < ne
        zero = jnp.sum(jnp.where(ffn, 0.0, gate), axis=1, keepdims=True)
        wt = jnp.where(ffn, gate, 0.0).reshape(t * top)
        h = _combine(ret, y, f, u, pos, wt, zero, top)
        return h.reshape(rows, seq, d)

    return jax.shard_map(body, mesh=mesh, in_specs=(tok, tok) + (rep,) * 13 + (espec,) * 3, out_specs=tok, check_vma=False)
```

```python
import functools

import jax
import jax.numpy as jnp
from jax import lax
from jax.experimental import pallas as pl
from jax.experimental.pallas import tpu as pltpu
from jax.sharding import PartitionSpec as P

NOPE = 128
ROPE = 64
EPS = 1e-6
SCALE = (NOPE + ROPE) ** -0.5
F32 = jnp.float32
BF16 = jnp.bfloat16
LANE = 128
VMEM_MAX = 67043328


def _rms(v, g):
    vf = v.astype(F32)
    return (vf * lax.rsqrt(jnp.mean(vf * vf, axis=-1, keepdims=True) + EPS) * g.astype(F32)).astype(BF16)


def _rope(v, cos, sin):
    half = ROPE // 2
    v1 = v[..., :half]
    v2 = v[..., half:]
    return jnp.concatenate([v1 * cos - v2 * sin, v1 * sin + v2 * cos], axis=-1)


def _swiglu(z, wg, wu, wd):
    hid = jax.nn.silu(jnp.dot(z, wg, preferred_element_type=F32)) * jnp.dot(z, wu, preferred_element_type=F32)
    return jnp.dot(hid.astype(BF16), wd, preferred_element_type=F32).astype(BF16)


def _gates(u, ids, w_r):
    g = jax.nn.softmax(jnp.dot(u, w_r, preferred_element_type=F32), axis=-1)
    hit = ids[:, :, None] == jnp.arange(g.shape[1], dtype=ids.dtype)
    sel = jnp.sum(jnp.where(hit, g[:, None, :], 0.0), axis=2)
    return sel / jnp.sum(sel, axis=1, keepdims=True)


def _rope_tables(pos):
    half = ROPE // 2
    ang = pos.astype(F32)[:, None] * (10000.0 ** (-jnp.arange(half, dtype=F32) / half))[None, :]
    return jnp.cos(ang), jnp.sin(ang)


def _attn_kernel(off_ref, qt_ref, qr_ref, kv_ref, o_ref):
    hg, seq, r = qt_ref.shape
    blocks = kv_ref.shape[0]
    keys = blocks * seq
    kv = kv_ref[...].reshape(keys, kv_ref.shape[-1])
    c = kv[:, :r]
    kr = kv[:, r:]
    nt = (((1,), (1,)), ((), ()))
    s = lax.dot_general(qt_ref[...].reshape(hg * seq, r), c, nt, preferred_element_type=F32)
    s = s + lax.dot_general(qr_ref[...].reshape(hg * seq, qr_ref.shape[-1]), kr, nt, preferred_element_type=F32)
    s = (s * SCALE).reshape(hg, seq, keys)
    query = off_ref[0] + lax.broadcasted_iota(jnp.int32, (1, seq, keys), 1)
    key = lax.broadcasted_iota(jnp.int32, (1, seq, keys), 2)
    s = jnp.where(key <= query, s, -jnp.inf).reshape(hg * seq, keys)
    p = jnp.exp(s - jnp.max(s, axis=-1, keepdims=True))
    den = jnp.sum(p, axis=-1, keepdims=True)
    lat = jnp.dot(p.astype(BF16), c, preferred_element_type=F32) / den
    o_ref[...] = lat.astype(BF16).reshape(hg, seq, r)


def _attention(off, qt, qr, kv, hg):
    heads, rows, seq, r = qt.shape
    e = qr.shape[-1]
    blocks = kv.shape[0]
    return pl.pallas_call(
        _attn_kernel,
        grid_spec=pltpu.PrefetchScalarGridSpec(
            num_scalar_prefetch=1,
            grid=(rows, heads // hg),
            in_specs=[
                pl.BlockSpec((hg, None, seq, r), lambda b, g, _: (g, b, 0, 0)),
                pl.BlockSpec((hg, None, seq, e), lambda b, g, _: (g, b, 0, 0)),
                pl.BlockSpec((blocks, None, seq, r + e), lambda b, g, _: (0, b, 0, 0)),
            ],
            out_specs=pl.BlockSpec((hg, None, seq, r), lambda b, g, _: (g, b, 0, 0)),
        ),
        out_shape=jax.ShapeDtypeStruct(qt.shape, BF16),
        compiler_params=pltpu.CompilerParams(vmem_limit_bytes=VMEM_MAX, dimension_semantics=("arbitrary", "arbitrary")),
        cost_estimate=pl.CostEstimate(
            flops=2 * heads * rows * seq * blocks * seq * (2 * r + e),
            bytes_accessed=2 * (2 * qt.size + qr.size + kv.size),
            transcendentals=heads * rows * seq * blocks * seq),
        name="latent_attention",
    )(off, qt, qr, kv)


def _pick_kernel(n, outs, steps, idx_ref, *rest):
    srcs, o_refs, buf, sem = rest[:n], rest[n:n + outs], rest[n + outs], rest[n + outs + 1]
    size = buf.shape[0] // n
    tile = o_refs[0].shape[0]
    step = 16
    at = pl.program_id(0)

    @pl.when(at == 0)
    def _():
        copies = [pltpu.make_async_copy(srcs[q], buf.at[pl.ds(q * size, size)], sem.at[q]) for q in range(n)]
        for c in copies:
            c.start()
        for c in copies:
            c.wait()

    for q, o_ref in enumerate(o_refs):
        @pl.when((at >= q * steps) & (at < (q + 1) * steps))
        def _(o_ref=o_ref):
            def some(i, _):
                base = pl.multiple_of(i * step, step)
                for a in range(step):
                    o_ref[base + a] = buf[idx_ref[at * tile + base + a]]
                return 0

            lax.fori_loop(0, tile // step, some, 0)


def _pick(srcs, idx, tile, outs):
    size, k, _ = srcs[0].shape
    rows = idx.shape[0]
    n = len(srcs)
    steps = rows // outs // tile
    return pl.pallas_call(
        functools.partial(_pick_kernel, n, outs, steps),
        grid_spec=pltpu.PrefetchScalarGridSpec(
            num_scalar_prefetch=1,
            grid=(rows // tile,),
            in_specs=[pl.BlockSpec(memory_space=pl.ANY)] * n,
            out_specs=[pl.BlockSpec((tile, k, LANE), lambda i, *_, q=q: (jnp.clip(i - q * steps, 0, steps - 1), 0, 0)) for q in range(outs)],
            scratch_shapes=[pltpu.VMEM((n * size, k, LANE), BF16), pltpu.SemaphoreType.DMA((n,))],
        ),
        out_shape=[jax.ShapeDtypeStruct((rows // outs, k, LANE), BF16)] * outs,
        compiler_params=pltpu.CompilerParams(vmem_limit_bytes=VMEM_MAX, dimension_semantics=("arbitrary",)),
        cost_estimate=pl.CostEstimate(flops=10**9, bytes_accessed=2 * (n * size + rows) * k * LANE, transcendentals=0),
    )(idx, *srcs)


def _tables(ids, experts, per):
    k = jnp.arange(ids.shape[-1], dtype=jnp.int32)
    hit = jnp.any(ids[:, None] == experts[None, :, None, None], axis=2)
    tri = (k[:, None] < k[None, :]).astype(BF16)
    pre = jnp.einsum('nmt,ts->nms', hit.astype(BF16), tri, preferred_element_type=F32).astype(jnp.int32)
    rank = jnp.where(hit, pre, -1)
    return jnp.sum(jnp.where(rank[:, :, None, :] == jnp.arange(per)[:, None], k, 0), axis=-1)


def _expert_kernel(nb, b_ref, xa_ref, *rest):
    xb_refs, (wg_ref, wu_ref, wd_ref, o_ref) = rest[:nb], rest[nb:]
    per = xa_ref.shape[2]
    half = xa_ref.shape[3] * LANE
    xa = xa_ref[...].reshape(nb * per, half)
    xb = jnp.concatenate([r[...].reshape(per, half) for r in xb_refs], axis=0)

    def proj(w_ref):
        return (jnp.dot(xa, w_ref[:half], preferred_element_type=F32)
                + jnp.dot(xb, w_ref[half:], preferred_element_type=F32))

    g = proj(wg_ref)
    hid = (jax.nn.silu(g) * proj(wu_ref)).astype(BF16)
    o = jnp.dot(hid, wd_ref[...], preferred_element_type=F32).astype(BF16)
    for q in range(nb):
        o_ref[lax.rem(b_ref[0] + nb - q, nb), 0] = o[q * per:(q + 1) * per].reshape(o_ref.shape[2:])


def _expert(b, xa, xb, w_eg, w_eu, w_ed, e):
    ncp, nb, per, k, _ = xa.shape
    d, f = w_eg.shape[1:]
    one = pl.Buffered(1)
    wspec = lambda s: pl.BlockSpec((None,) + s, lambda i, *_: (e, 0, 0), pipeline_mode=one)
    cap = ncp * nb * per
    return pl.pallas_call(
        functools.partial(_expert_kernel, nb),
        grid_spec=pltpu.PrefetchScalarGridSpec(
            num_scalar_prefetch=1,
            grid=(ncp,),
            in_specs=[pl.BlockSpec((1, nb, per, k, LANE), lambda i, *_: (i, 0, 0, 0, 0))]
            + [pl.BlockSpec((1, per, k, LANE), lambda i, *_: (i, 0, 0, 0))] * nb
            + [wspec((d, f)), wspec((d, f)), wspec((f, d))],
            out_specs=pl.BlockSpec((nb, 1, per, d // LANE, LANE), lambda i, *_: (0, i, 0, 0, 0)),
        ),
        out_shape=jax.ShapeDtypeStruct((nb, ncp, per, d // LANE, LANE), BF16),
        compiler_params=pltpu.CompilerParams(vmem_limit_bytes=VMEM_MAX, dimension_semantics=("arbitrary",)),
        cost_estimate=pl.CostEstimate(flops=6 * cap * d * f, bytes_accessed=6 * d * f + 4 * cap * d, transcendentals=cap * f),
    )(b, xa, *xb, w_eg, w_eu, w_ed)


def _combine_kernel(top, pos_ref, gate_ref, z_ref, y_ref, f_ref, u_ref, *rest):
    epd = len(rest) - 3
    rets, o_ref, buf, sem = rest[:epd], rest[epd], rest[epd + 1], rest[epd + 2]
    cap = rets[0].shape[0]
    tb, d = y_ref.shape
    k = d // LANE
    step = 16

    @pl.when(pl.program_id(0) == 0)
    def _():
        copies = [pltpu.make_async_copy(rets[s], buf.at[pl.ds(s * cap, cap)], sem.at[s]) for s in range(epd)]
        for c in copies:
            c.start()
        buf[pl.ds(epd * cap, 8)] = jnp.zeros((8, k, LANE), BF16)
        for c in copies:
            c.wait()

    first = pl.program_id(0) * tb

    def tok(i, _):
        base = pl.multiple_of(i * step, step)
        accs = []
        for a in range(step):
            acc = None
            for j in range(top):
                q = (first + base + a) * top + j
                term = buf[pos_ref[q]].astype(F32) * gate_ref[q]
                acc = term if acc is None else acc + term
            accs.append(acc)
        m = jnp.stack(accs).reshape(step, d)
        sl = pl.ds(base, step)
        m = m + z_ref[sl, :] * u_ref[sl, :].astype(F32)
        o_ref[sl, :] = (y_ref[sl, :].astype(F32) + f_ref[sl, :].astype(F32) + m).astype(BF16)
        return 0

    lax.fori_loop(0, tb // step, tok, 0)


def _combine(rets, y, f, u, pos, gate, zero, top):
    t, d = y.shape
    cap, k, _ = rets[0].shape
    epd = len(rets)
    tb = 128
    row = pl.BlockSpec((tb, d), lambda i, *_: (i, 0))
    return pl.pallas_call(
        functools.partial(_combine_kernel, top),
        grid_spec=pltpu.PrefetchScalarGridSpec(
            num_scalar_prefetch=2,
            grid=(t // tb,),
            in_specs=[pl.BlockSpec((tb, 1), lambda i, *_: (i, 0)), row, row, row] + [pl.BlockSpec(memory_space=pl.ANY)] * epd,
            out_specs=row,
            scratch_shapes=[pltpu.VMEM((epd * cap + 8, k, LANE), BF16), pltpu.SemaphoreType.DMA((epd,))],
        ),
        out_shape=jax.ShapeDtypeStruct((t, d), BF16),
        compiler_params=pltpu.CompilerParams(vmem_limit_bytes=VMEM_MAX, dimension_semantics=("arbitrary",)),
        cost_estimate=pl.CostEstimate(flops=2 * 10**9, bytes_accessed=2 * (epd * cap + 4 * t) * d, transcendentals=0),
        name="combine_rows",
    )(pos, gate, zero, y, f, u, *rets)


def solution(mesh):
    ncp = mesh.shape['cp']
    nb = mesh.shape['b']
    ngroup = nb * ncp
    axes = ('b', 'cp')
    tok = P(('dp', 'b'), 'cp', None)
    rep = P()
    espec = P(('b', 'cp'), None, None)

    def body(x, ids, g_attn, w_q, w_dkv, w_kr, w_uk, w_uv, w_o, g_ffn, w_fg, w_fu, w_fd, g_moe, w_r, w_eg, w_eu, w_ed):
        rows, seq, d = x.shape
        heads, r, vd = w_uv.shape
        top = ids.shape[-1]
        t = rows * seq
        epd = w_eg.shape[0]
        ne = epd * ngroup
        hot = (w_r.shape[1] // top) // 2
        per = (t + hot - 1) // hot
        cap = ngroup * per
        i = lax.axis_index('cp')
        xt = x.reshape(t, d)
        idf = ids.reshape(t, top)

        b = lax.axis_index('b')
        oh = idf[:, :, None] == jnp.arange(ne, dtype=idf.dtype)
        hit = jnp.any(oh, axis=1)
        k = jnp.arange(t)
        tri = (k[:, None] > k[None, :]).astype(BF16)
        pre = jnp.dot(tri, hit.astype(BF16), preferred_element_type=F32).astype(jnp.int32)
        ids_t = idf.T
        ids_b = lax.all_gather(ids_t, 'b')
        ids_c = lax.all_gather(ids_t, 'cp')
        xt_moe, ids_b, ids_c = lax.optimization_barrier((xt, ids_b, ids_c))
        turn = jnp.arange(nb, dtype=jnp.int32)
        loc_e = jnp.arange(epd, dtype=jnp.int32)
        exp_a = b * ncp * epd + jnp.arange(ncp * epd, dtype=jnp.int32)
        exp_b = (((turn[:, None] * ncp + i) * epd) + loc_e).reshape(-1)
        tab_b = _tables(ids_b, exp_a, per).reshape(nb, ncp, epd, per)[(b + nb - turn) % nb]
        idx_a = jnp.transpose(tab_b + (turn * t)[:, None, None, None], (2, 1, 0, 3)).reshape(epd, -1)
        tab_c = _tables(ids_c, exp_b, per).reshape(ncp, nb, epd, per)[:, (b + turn) % nb]
        idx_b = jnp.transpose(tab_c + (jnp.arange(ncp, dtype=jnp.int32) * t)[:, None, None, None], (2, 1, 0, 3)).reshape(epd, -1)

        u = _rms(xt_moe, g_moe)
        kk = d // LANE // 2
        u_a = u[:, :d // 2].reshape(t, kk, LANE)
        u_b = u[:, d // 2:].reshape(t, kk, LANE)
        all_b = lax.all_gather(u_b, 'cp')
        near = [u_a] + [lax.ppermute(u_a, 'b', [(p, (p + q) % nb) for p in range(nb)]) for q in range(1, nb)]
        all_b = all_b.reshape(ncp * t, kk, LANE)
        got = []
        for s in range(epd):
            send_a = _pick(near, idx_a[s], nb * per, 1)[0].reshape(ncp, nb, per, kk, LANE)
            send_b = [o.reshape(ncp, per, kk, LANE) for o in _pick([all_b], idx_b[s], nb * per, nb)]
            if s:
                send_a, send_b, _, _ = lax.optimization_barrier((send_a, send_b, got[-1][0], got[-1][1][1]))
            got_a = lax.all_to_all(send_a, 'cp', 0, 0)
            got_b = [send_b[0]]
            for q in range(1, nb):
                got_b.append(lax.ppermute(send_b[q], 'b', [(p, (p + q) % nb) for p in range(nb)]))
            got.append((got_a, got_b))

        off = i * seq
        cos, sin = _rope_tables(off + jnp.arange(seq))
        n = _rms(xt, g_attn)
        c = jnp.dot(n, w_dkv, preferred_element_type=F32).astype(BF16).reshape(rows, seq, r)
        kr = _rope(jnp.dot(n, w_kr, preferred_element_type=F32).reshape(rows, seq, ROPE), cos, sin).astype(BF16)
        kv = lax.all_gather(jnp.concatenate([c, kr], axis=-1), 'cp')

        ex = jnp.arange(ne, dtype=jnp.int32)
        at = pre + ((ex % epd) * cap + (ex // epd) * per)[None, :]
        pos = jnp.sum(jnp.where(oh, at[:, None, :], 0), axis=2)
        pos = jnp.where(idf < ne, pos, epd * cap).reshape(t * top)

        w_qh = w_q.reshape(d, heads, NOPE + ROPE)
        qn = jnp.dot(n, w_qh[..., :NOPE].reshape(d, heads * NOPE), preferred_element_type=F32).astype(BF16)
        qr = jnp.dot(n, w_qh[..., NOPE:].reshape(d, heads * ROPE), preferred_element_type=F32)
        qr = jnp.transpose(qr.reshape(rows, seq, heads, ROPE), (2, 0, 1, 3))
        qr = _rope(qr, cos, sin).astype(BF16)
        qt = jnp.einsum('thn,hnr->htr', qn.reshape(t, heads, NOPE), w_uk, preferred_element_type=F32).astype(BF16)
        lat = _attention(jnp.reshape(off, (1,)).astype(jnp.int32), qt.reshape(heads, rows, seq, r), qr, kv, heads // 2)
        o = jnp.einsum('htr,hrv->thv', lat.reshape(heads, t, r), w_uv, preferred_element_type=F32).astype(BF16)
        a = jnp.dot(o.reshape(t, heads * vd), w_o, preferred_element_type=F32).astype(BF16)
        y = (xt.astype(F32) + a.astype(F32)).astype(BF16)
        f = _swiglu(_rms(y, g_ffn), w_fg, w_fu, w_fd)

        gate = _gates(u, idf, w_r)
        ret = []
        for s in range(epd):
            out = _expert(jnp.reshape(b, (1,)).astype(jnp.int32), got[s][0], got[s][1], w_eg, w_eu, w_ed, s)
            ret.append(lax.all_to_all(out.reshape(ngroup, per, d // LANE, LANE), axes, 0, 0).reshape(cap, d // LANE, LANE))
        ffn = idf < ne
        zero = jnp.sum(jnp.where(ffn, 0.0, gate), axis=1, keepdims=True)
        wt = jnp.where(ffn, gate, 0.0).reshape(t * top)
        h = _combine(ret, y, f, u, pos, wt, zero, top)
        return h.reshape(rows, seq, d)

    return jax.shard_map(body, mesh=mesh, in_specs=(tok, tok) + (rep,) * 13 + (espec,) * 3, out_specs=tok, check_vma=False)
```
